32 devices in a mesh: role: 2 (over core), dev: 16 (over z, y, x).
Axes of the slice: x: 2, y: 2, z: 4, core: 2. Of those that a mesh axis runs over, the one named last changes fastest.
Arguments:
- table_rows: bfloat16 [32, 2048, 128], P('dev'), may hold values from -6 to 6
- piece_table: int32 [32], replicated, may hold values from 0 to 25, as said below
- bag_rows: int32 [32, 8192], P('dev'), may hold values from 0 to 2047
- bag_of: int32 [32, 8192], P('dev'), may hold values from 0 to 4095, never falling along the last dimension, each value on 1 to 8 neighbouring positions
- bag_weight: bfloat16 [32, 8192], P('dev'), may hold values from 0.25 to 2
- dense_input: bfloat16 [4096, 128], P('dev'), may hold values from -6 to 6
- labels: float32 [4096], P('dev'), may hold values from 0 to 1
- cross_u: bfloat16 [3456, 512], replicated, may hold values from -0.109375 to 0.109375
- cross_v: bfloat16 [512, 3456], replicated, may hold values from -0.25 to 0.25
- cross_bias: float32 [3456], replicated, may hold values from -3 to 3
- top_w1: bfloat16 [3456, 1024], replicated, may hold values from -0.109375 to 0.109375
- top_b1: float32 [1024], replicated, may hold values from -3 to 3
- out_w: bfloat16 [1024], replicated, may hold values from -0.375 to 0.375
Outputs:
- piece_grads: bfloat16 [16, 256, 32, 128], P(None, 'role', 'dev')
The draws below stay inside these ranges and needn't reach their ends.
Inputs may be any that keep to these rules, and one draw needn't show every extreme that they name: `piece_table`: every one of the 26 tables owns one piece or more. `bag_of`: in each piece the bag numbers never fall along the lookups, and every sample has 1 to 8 lookups in every piece.
All inputs are finite; a program needn't handle non-finite values.
Results may differ from the reference program's by a relative error of at most 0.012.
The reference program's roundings to bfloat16 on the way count: a program that leaves them out, or rounds other values in their place, can miss the bound.
Values may be sent and summed in bfloat16 or wider, within the bound.
A program may use at most 128 MiB of HBM per device.

```python
import math
import jax
import jax.numpy as jnp
import numpy as np
from jax import lax

E = 128
TABLES = 26
RANK = 512
HIDDEN_SIZE = 1024
TOK_DEV = 256
ROWS_PIECE = 2048
MOST = 8
PIECES = 32
BATCH = 4096
LOOKS_PIECE = 8192
WIDTH = 3456
N_DEV = 16


def placement_helper(key):
    key_first = jax.random.fold_in(key, 11)
    key_second = jax.random.fold_in(key, 12)
    key_third = jax.random.fold_in(key, 13)
    leading = jax.random.permutation(key_first, TABLES).astype(jnp.int32)
    surplus = jax.random.randint(key_second, (PIECES - TABLES,), 0, TABLES).astype(jnp.int32)
    assigned = jnp.concatenate([leading, surplus])
    shuffle = jax.random.permutation(key_third, PIECES)
    return assigned[shuffle].astype(jnp.int32)


def draw_piece_table(key, part):
    return placement_helper(key)


def set_ends(values, key, least, top_value):
    dims = values.shape
    spot = [jax.random.randint(jax.random.fold_in(key, axis), (), 0, dims[axis]) for axis in range(len(dims))]
    values = values.at[tuple(spot)].set(least)
    longest = dims.index(max(dims))
    spot[longest] = (spot[longest] + 1) % dims[longest]
    return values.at[tuple(spot)].set(top_value)


def shard_levels(own_key, shape, cuts, smallest, high):
    gain = 1.0
    for axis_at, parts in cuts:
        heights = jax.random.uniform(jax.random.fold_in(jax.random.fold_in(own_key, 6), axis_at), (parts,), jnp.float32, smallest / len(cuts), high / len(cuts))
        gain = gain * jnp.repeat(jnp.exp(heights), shape[axis_at] // parts).reshape((-1,) + (1,) * (len(shape) - 1 - axis_at))
    return gain


def length_profile(amount, total, limit, skew):
    weights = [(1 << 20) // math.isqrt(grade ** skew) + 1 for grade in range(2, amount + 1)]
    rest, given = total - limit - (amount - 1), [1] * (amount - 1)
    while rest > 0:
        free = [i for i in range(amount - 1) if given[i] < limit]
        pool, budget = sum([weights[i] for i in free]), rest
        for i in free:
            extra = min(limit - given[i], max(1, budget * weights[i] // pool), rest)
            given[i] = given[i] + extra
            rest = rest - extra
    return np.array([limit] + given)


def ragged_sizes(stream_key, amount, total, most, lean):
    if amount == 2:
        one = jax.random.randint(stream_key, (), max(1, total - most), min(most, total - 1) + 1)
        return jnp.stack([one, total - one])
    lengths = jnp.asarray(length_profile(amount, total, most, lean), jnp.int32)
    pairs = (amount - 1) // 2
    donor, sink = lengths[1:1 + 2 * pairs:2], lengths[2:2 + 2 * pairs:2]
    margin = jnp.minimum(donor - 1, most - sink)
    passed = jax.random.randint(jax.random.fold_in(stream_key, 1), (pairs,), 0, 1 << 20) % (margin + 1)
    lengths = lengths.at[1:1 + 2 * pairs:2].set(donor - passed).at[2:2 + 2 * pairs:2].set(sink + passed)
    return lengths[jax.random.permutation(jax.random.fold_in(stream_key, 2), amount)]


def normal_values(key, shape, width, reach, split=(), dtype=jnp.bfloat16):
    entries = jax.random.normal(key, shape, jnp.float32) * width
    if len(split) > 0:
        entries = shard_levels(key, shape, split, -0.22, 0.18) * entries
    return jnp.clip(entries, min=-reach, max=reach).astype(dtype)


def setup_inputs(seed: int = 0) -> dict:
    key_list = jax.random.split(jax.random.key(seed), 14)
    return {
        "table_rows": normal_values(key_list[0], (PIECES, ROWS_PIECE, E), 1.0, 6.0, ((0, 16),)),
        "piece_table": draw_piece_table(jax.random.fold_in(key_list[13], 71), 0),
        "bag_rows": set_ends(jax.random.randint(key_list[2], (PIECES, LOOKS_PIECE), 0, ROWS_PIECE), jax.random.fold_in(key_list[2], 1), 0, ROWS_PIECE - 1).astype(jnp.int32),
        "bag_of": jax.vmap(lambda own: jnp.searchsorted(jnp.cumsum(ragged_sizes(own, BATCH, LOOKS_PIECE, MOST, 2)), jnp.arange(LOOKS_PIECE), side="right"))(jax.random.split(key_list[3], PIECES)).reshape((PIECES, LOOKS_PIECE)).astype(jnp.int32),
        "bag_weight": jnp.clip(jnp.exp(math.log(2.0) - 2.0794415 * jax.random.uniform(key_list[4], (PIECES, LOOKS_PIECE), jnp.float32) ** shard_levels(key_list[4], (PIECES, LOOKS_PIECE), ((0, 16),), -0.2, 0.2)), 0.25, 2.0).astype(jnp.bfloat16),
        "dense_input": normal_values(key_list[5], (BATCH, E), 1.0, 6.0, ((0, 16),)),
        "labels": jnp.clip(1.0 * jax.random.uniform(key_list[6], (BATCH,), jnp.float32) ** shard_levels(key_list[6], (BATCH,), ((0, 16),), -0.2, 0.2), 0.0, 1.0),
        "cross_u": normal_values(key_list[7], (WIDTH, RANK), WIDTH ** -0.5, 0.109375),
        "cross_v": normal_values(key_list[8], (RANK, WIDTH), RANK ** -0.5, 0.25),
        "cross_bias": normal_values(key_list[9], (WIDTH,), 0.5, 3.0, (), jnp.float32),
        "top_w1": normal_values(key_list[10], (WIDTH, HIDDEN_SIZE), WIDTH ** -0.5, 0.109375),
        "top_b1": normal_values(key_list[11], (HIDDEN_SIZE,), 0.5, 3.0, (), jnp.float32),
        "out_w": normal_values(key_list[12], (HIDDEN_SIZE,), (HIDDEN_SIZE // 4) ** -0.5, 0.375),
    }


def dense_grads(pooled, dense_in, label_rows, cross_u, cross_v, cross_bias, top_w1, top_b1, out_w):
    row_count = pooled.shape[0]
    embed_width = dense_in.shape[1]
    features = jnp.concatenate([dense_in.astype(jnp.float32)[:, None, :], pooled], axis=1).reshape(row_count, -1)
    low_rank = jnp.dot(features.astype(jnp.bfloat16), cross_u, preferred_element_type=jnp.float32).astype(jnp.bfloat16)
    cross_out = jnp.dot(low_rank, cross_v, preferred_element_type=jnp.float32) + cross_bias
    mixed = (features * cross_out + features).astype(jnp.bfloat16)
    pre_act = jnp.dot(mixed, top_w1, preferred_element_type=jnp.float32) + top_b1
    out_weight = out_w.astype(jnp.float32)
    sig_act = jax.nn.sigmoid(pre_act)
    logits = jnp.sum(pre_act * sig_act * out_weight, axis=1)
    grad_logit = jax.nn.sigmoid(logits) - label_rows
    slope = sig_act * (1.0 + pre_act * (1.0 - sig_act))
    grad_act = (grad_logit[:, None] * out_weight * slope).astype(jnp.bfloat16)
    grad_mixed = jnp.dot(grad_act, top_w1.T, preferred_element_type=jnp.float32)
    grad_cross = (grad_mixed * features).astype(jnp.bfloat16)
    grad_low = jnp.dot(grad_cross, cross_v.T, preferred_element_type=jnp.float32).astype(jnp.bfloat16)
    grad_features = grad_mixed * (cross_out + 1.0) + jnp.dot(grad_low, cross_u.T, preferred_element_type=jnp.float32)
    return grad_features.reshape(row_count, -1, embed_width)[:, 1:, :].astype(jnp.bfloat16)


def reference(table_rows, piece_table, bag_rows, bag_of, bag_weight, dense_input, labels, cross_u, cross_v, cross_bias, top_w1, top_b1, out_w):
    def add_piece(pooled, element):
        piece_rows, table_id, row_ids, bag_ids, weights = element
        picked = piece_rows[row_ids].astype(jnp.float32)
        summed = jax.ops.segment_sum(picked * weights.astype(jnp.float32)[:, None], bag_ids, num_segments=BATCH)
        rounded = lax.optimization_barrier(summed.astype(jnp.bfloat16)).astype(jnp.float32)
        current = lax.dynamic_index_in_dim(pooled, table_id, 1, keepdims=False)
        return lax.dynamic_update_index_in_dim(pooled, current + rounded, table_id, 1), None

    pooled, _ = lax.scan(add_piece, jnp.zeros((BATCH, TABLES, E), jnp.float32), (table_rows, piece_table, bag_rows, bag_of, bag_weight))
    grad_pooled = dense_grads(pooled, dense_input, labels, cross_u, cross_v, cross_bias, top_w1, top_b1, out_w)
    selected = jnp.take(grad_pooled, piece_table, axis=1)
    return selected.reshape(N_DEV, TOK_DEV, PIECES, E)
```

```python
import functools

import jax
import jax.numpy as jnp
from jax import lax
from jax.experimental import pallas as pl
from jax.experimental.pallas import tpu as pltpu
from jax.sharding import PartitionSpec as P

LANES = 128
WINDOW = 256
LOW = 256
NT = (((1,), (1,)), ((), ()))
NN = (((1,), (0,)), ((), ()))


def dot(a, b, dims=NN):
    return lax.dot_general(a, b, dims, preferred_element_type=jnp.float32)


def pool_kernel(first_ref, last_ref, table_ref, rows_ref, bags_ref, scale_ref, out_ref, flipped, scale_wide):
    blocks, pieces, half, width = out_ref.shape
    length = table_ref.shape[1]
    total = rows_ref.shape[1]
    groups = length // LOW
    role = lax.axis_index("role")
    scale_wide[...] = scale_ref[...].astype(jnp.float32)
    for p in range(pieces):
        for g in range(groups):
            flipped[p, g * width : (g + 1) * width, :] = (
                table_ref[p, g * LOW : (g + 1) * LOW, :].astype(jnp.float32).T.astype(jnp.bfloat16)
            )
    low_ids = lax.broadcasted_iota(jnp.int32, (LOW, WINDOW), 0)
    bag_ids = lax.broadcasted_iota(jnp.int32, (half, WINDOW), 0)
    places = lax.broadcasted_iota(jnp.int32, (1, WINDOW), 1)

    def window(p, base, begin, first_bag):
        start = pl.multiple_of(jnp.minimum(begin, total - WINDOW), LANES)
        span = pl.ds(start, WINDOW)
        ids = rows_ref[pl.ds(p, 1), span]
        bags = bags_ref[pl.ds(p, 1), span] - first_bag
        bags = jnp.where(places + start >= begin, bags, -1)
        scale = scale_wide[pl.ds(p, 1), span]
        low, high = ids % LOW, ids // LOW
        hot = jnp.where(low_ids == low, 1.0, 0.0).astype(jnp.bfloat16)
        candidates = dot(flipped[p], hot)
        picked = candidates[:width]
        for g in range(1, groups):
            picked = jnp.where(high == g, candidates[g * width : (g + 1) * width], picked)
        spread = jnp.where(bag_ids == bags, scale, 0.0).astype(jnp.bfloat16)
        return dot(spread, picked.astype(jnp.bfloat16), NT)

    for p in range(pieces):

        @pl.loop(0, blocks)
        def _(k):
            first_bag = (2 * k + role) * half
            base = first_ref[p, k] // LANES * LANES
            count = (last_ref[p, k] - base + WINDOW - 1) // WINDOW

            def more(j, acc):
                return acc + window(p, base, base + j * WINDOW, first_bag)

            acc = window(p, base, base, first_bag)
            acc = lax.fori_loop(1, count, more, acc)
            out_ref[k, p] = acc.astype(jnp.bfloat16)


def pool(table_rows, bag_rows, bag_of, bag_weight, half, blocks):
    pieces, length, width = table_rows.shape
    role = lax.axis_index("role")
    edges = (2 * jnp.arange(blocks, dtype=jnp.int32) + role) * half
    first = jnp.sum((bag_of[:, None, :] < edges[None, :, None]).astype(jnp.int32), axis=2)
    last = jnp.sum((bag_of[:, None, :] < edges[None, :, None] + half).astype(jnp.int32), axis=2)
    vmem = pl.BlockSpec(memory_space=pltpu.VMEM)
    smem = pl.BlockSpec(memory_space=pltpu.SMEM)
    return pl.pallas_call(
        pool_kernel,
        out_shape=jax.ShapeDtypeStruct((blocks, pieces, half, width), jnp.bfloat16),
        in_specs=[smem, smem, vmem, vmem, vmem, vmem],
        out_specs=vmem,
        scratch_shapes=[
            pltpu.VMEM((pieces, length // LOW * width, LOW), jnp.bfloat16),
            pltpu.VMEM(bag_weight.shape, jnp.float32),
        ],
        compiler_params=pltpu.CompilerParams(vmem_limit_bytes=40 * 1024 * 1024),
    )(first, last, table_rows, bag_rows, bag_of, bag_weight)


def dense_kernel(
    owner_ref, arrived_ref, dense_ref, label_ref, bias_ref, b1_ref, out_w_ref, u_hbm, v_hbm, w_hbm,
    out_ref, u_ref, v_ref, w_ref, feats, crossed, mixed_grad, grads, sems,
):
    pieces, rows, width = arrived_ref.shape
    wide = feats.shape[1]
    role = lax.axis_index("role")
    load_u = pltpu.make_async_copy(u_hbm, u_ref, sems.at[0])
    load_v = pltpu.make_async_copy(v_hbm, v_ref, sems.at[1])
    load_w = pltpu.make_async_copy(w_hbm, w_ref, sems.at[2])
    load_u.start()
    load_v.start()
    load_w.start()

    feats[...] = jnp.zeros_like(feats)
    feats[:, :width] = dense_ref[pl.ds(pl.multiple_of(role * rows, rows), rows), :].astype(jnp.float32)

    @pl.loop(0, pieces)
    def _(p):
        at = pl.ds(pl.multiple_of((owner_ref[p] + 1) * width, width), width)
        feats[:, at] = feats[:, at] + arrived_ref[p].astype(jnp.float32)

    step = next(n for n in (3 * width, width) if wide % n == 0)
    parts = [slice(i, i + step) for i in range(0, wide, step)]

    load_u.wait()
    low_rank = dot(feats[...].astype(jnp.bfloat16), u_ref[...]).astype(jnp.bfloat16)
    load_v.wait()
    load_w.wait()
    pre_act = b1_ref[...]
    for part in parts:
        cross_out = dot(low_rank, v_ref[:, part]) + bias_ref[:, part]
        crossed[:, part] = cross_out
        own = feats[:, part]
        pre_act = pre_act + dot((own * cross_out + own).astype(jnp.bfloat16), w_ref[part, :])
    out_weight = out_w_ref[...].astype(jnp.float32)
    sig_act = jax.nn.sigmoid(pre_act)
    logits = jnp.sum(pre_act * sig_act * out_weight, axis=1, keepdims=True)
    row_at = lax.broadcasted_iota(jnp.int32, (rows, rows), 0)
    column_at = lax.broadcasted_iota(jnp.int32, (rows, rows), 1)
    labels = jnp.sum(
        jnp.where(row_at == column_at, label_ref[pl.ds(role, 1), :], 0.0), axis=1, keepdims=True
    )
    grad_logit = jax.nn.sigmoid(logits) - labels
    slope = sig_act * (1.0 + pre_act * (1.0 - sig_act))
    grad_act = (grad_logit * out_weight * slope).astype(jnp.bfloat16)
    grad_low = jnp.zeros((rows, u_ref.shape[1]), jnp.float32)
    for part in parts:
        grad_mixed = dot(grad_act, w_ref[part, :], NT)
        grad_cross = (grad_mixed * feats[:, part]).astype(jnp.bfloat16)
        mixed_grad[:, part] = grad_mixed * (crossed[:, part] + 1.0)
        grad_low = grad_low + dot(grad_cross, v_ref[:, part], NT)
    grad_low = grad_low.astype(jnp.bfloat16)
    for part in parts:
        total = (mixed_grad[:, part] + dot(grad_low, u_ref[part, :], NT)).astype(jnp.bfloat16)
        for i in range(step // width):
            grads[part.start // width + i] = total[:, i * width : (i + 1) * width]

    @pl.loop(0, pieces)
    def _(p):
        out_ref[p] = grads[owner_ref[p] + 1]


def dense(arrived, piece_table, dense_input, labels, cross_u, cross_v, cross_bias, top_w1, top_b1, out_w):
    pieces, rows, width = arrived.shape
    wide, rank = cross_u.shape
    hidden = top_w1.shape[1]
    vmem = pl.BlockSpec(memory_space=pltpu.VMEM)
    smem = pl.BlockSpec(memory_space=pltpu.SMEM)
    anywhere = pl.BlockSpec(memory_space=pl.ANY)
    return pl.pallas_call(
        dense_kernel,
        out_shape=jax.ShapeDtypeStruct(arrived.shape, jnp.bfloat16),
        in_specs=[smem] + [vmem] * 6 + [anywhere] * 3,
        out_specs=vmem,
        scratch_shapes=[
            pltpu.VMEM(cross_u.shape, jnp.bfloat16),
            pltpu.VMEM(cross_v.shape, jnp.bfloat16),
            pltpu.VMEM(top_w1.shape, jnp.bfloat16),
            pltpu.VMEM((rows, wide), jnp.float32),
            pltpu.VMEM((rows, wide), jnp.float32),
            pltpu.VMEM((rows, wide), jnp.float32),
            pltpu.VMEM((wide // width, rows, width), jnp.bfloat16),
            pltpu.SemaphoreType.DMA((3,)),
        ],
        compiler_params=pltpu.CompilerParams(vmem_limit_bytes=56 * 1024 * 1024),
    )(
        piece_table, arrived, dense_input, labels.reshape(2, rows), cross_bias[None], top_b1[None],
        out_w[None], cross_u, cross_v, top_w1,
    )


def local(
    table_rows, piece_table, bag_rows, bag_of, bag_weight, dense_input, labels,
    cross_u, cross_v, cross_bias, top_w1, top_b1, out_w,
):
    devices = lax.axis_size("dev")
    half = dense_input.shape[0] // 2
    pieces, _, width = table_rows.shape
    pooled = pool(table_rows, bag_rows, bag_of, bag_weight, half, devices)
    arrived = lax.all_to_all(pooled, "dev", split_axis=0, concat_axis=0, tiled=True)
    arrived = arrived.reshape(devices * pieces, half, width)
    grads = dense(
        arrived, piece_table, dense_input, labels, cross_u, cross_v, cross_bias, top_w1, top_b1, out_w
    )
    grads = grads.reshape(devices, pieces, half, width)
    returned = lax.all_to_all(grads, "dev", split_axis=0, concat_axis=0, tiled=True)
    return returned.transpose(0, 2, 1, 3)


def solution(mesh):
    split, whole = P("dev"), P()
    return jax.shard_map(
        local,
        mesh=mesh,
        in_specs=(split, whole, split, split, split, split, split) + (whole,) * 6,
        out_specs=P(None, "role", "dev", None),
        check_vma=False,
    )
```

```python
import functools

import jax
import jax.numpy as jnp
from jax import lax
from jax.experimental import pallas as pl
from jax.experimental.pallas import tpu as pltpu
from jax.sharding import PartitionSpec as P

LANES = 128
WINDOW = 384
LOW = 256
NT = (((1,), (1,)), ((), ()))
NN = (((1,), (0,)), ((), ()))


def dot(a, b, dims=NN):
    return lax.dot_general(a, b, dims, preferred_element_type=jnp.float32)


def pool_kernel(first_ref, last_ref, table_ref, rows_ref, bags_ref, scale_ref, out_ref, flipped, scale_wide):
    blocks, pieces, half, width = out_ref.shape
    length = table_ref.shape[1]
    total = rows_ref.shape[1]
    groups = length // LOW
    role = lax.axis_index("role")
    scale_wide[...] = scale_ref[...].astype(jnp.float32)
    for p in range(pieces):
        for g in range(groups):
            flipped[p, g * width : (g + 1) * width, :] = (
                table_ref[p, g * LOW : (g + 1) * LOW, :].astype(jnp.float32).T.astype(jnp.bfloat16)
            )
    low_ids = lax.broadcasted_iota(jnp.int32, (LOW, WINDOW), 0)
    bag_ids = lax.broadcasted_iota(jnp.int32, (half, WINDOW), 0)
    places = lax.broadcasted_iota(jnp.int32, (1, WINDOW), 1)

    def window(p, base, begin, first_bag):
        start = pl.multiple_of(jnp.minimum(begin, total - WINDOW), LANES)
        span = pl.ds(start, WINDOW)
        ids = rows_ref[pl.ds(p, 1), span]
        bags = bags_ref[pl.ds(p, 1), span] - first_bag
        bags = jnp.where(places + start >= begin, bags, -1)
        scale = scale_wide[pl.ds(p, 1), span]
        low, high = ids % LOW, ids // LOW
        hot = jnp.where(low_ids == low, 1.0, 0.0).astype(jnp.bfloat16)
        picked = dot(flipped[p, :width, :], hot)
        for g in range(1, groups):
            picked = jnp.where(high == g, dot(flipped[p, g * width : (g + 1) * width, :], hot), picked)
        spread = jnp.where(bag_ids == bags, scale, 0.0).astype(jnp.bfloat16)
        return dot(spread, picked.astype(jnp.bfloat16), NT)

    @pl.loop(0, blocks)
    def _(k):
        first_bag = (2 * k + role) * half
        bases = [first_ref[p, k] // LANES * LANES for p in range(pieces)]
        sums = [window(p, bases[p], bases[p], first_bag) for p in range(pieces)]
        for p in range(pieces):
            out_ref[k, p] = sums[p].astype(jnp.bfloat16)
        for p in range(pieces):
            count = (last_ref[p, k] - bases[p] + WINDOW - 1) // WINDOW

            @pl.when(count > 1)
            def _():
                def more(j, acc):
                    return acc + window(p, bases[p], bases[p] + j * WINDOW, first_bag)

                first = window(p, bases[p], bases[p], first_bag)
                out_ref[k, p] = lax.fori_loop(1, count, more, first).astype(jnp.bfloat16)


def pool(table_rows, bag_rows, bag_of, bag_weight, half, blocks):
    pieces, length, width = table_rows.shape
    role = lax.axis_index("role")
    edges = (2 * jnp.arange(blocks, dtype=jnp.int32) + role) * half
    first = jnp.sum((bag_of[:, None, :] < edges[None, :, None]).astype(jnp.int32), axis=2)
    last = jnp.sum((bag_of[:, None, :] < edges[None, :, None] + half).astype(jnp.int32), axis=2)
    vmem = pl.BlockSpec(memory_space=pltpu.VMEM)
    smem = pl.BlockSpec(memory_space=pltpu.SMEM)
    return pl.pallas_call(
        pool_kernel,
        out_shape=jax.ShapeDtypeStruct((blocks, pieces, half, width), jnp.bfloat16),
        in_specs=[smem, smem, vmem, vmem, vmem, vmem],
        out_specs=vmem,
        scratch_shapes=[
            pltpu.VMEM((pieces, length // LOW * width, LOW), jnp.bfloat16),
            pltpu.VMEM(bag_weight.shape, jnp.float32),
        ],
        compiler_params=pltpu.CompilerParams(vmem_limit_bytes=40 * 1024 * 1024),
    )(first, last, table_rows, bag_rows, bag_of, bag_weight)


def dense_kernel(
    owner_ref, arrived_ref, dense_ref, label_ref, bias_ref, b1_ref, out_w_ref, u_hbm, v_hbm, w_hbm,
    out_ref, u_ref, v_ref, w_ref, feats, crossed, mixed_grad, grads, sems,
):
    pieces, rows, width = arrived_ref.shape
    wide = feats.shape[1]
    role = lax.axis_index("role")
    load_u = pltpu.make_async_copy(u_hbm, u_ref, sems.at[0])
    load_v = pltpu.make_async_copy(v_hbm, v_ref, sems.at[1])
    load_w = pltpu.make_async_copy(w_hbm, w_ref, sems.at[2])
    load_u.start()
    load_v.start()
    load_w.start()

    feats[...] = jnp.zeros_like(feats)
    feats[:, :width] = dense_ref[pl.ds(pl.multiple_of(role * rows, rows), rows), :].astype(jnp.float32)

    @pl.loop(0, pieces)
    def _(p):
        at = pl.ds(pl.multiple_of((owner_ref[p] + 1) * width, width), width)
        feats[:, at] = feats[:, at] + arrived_ref[p].astype(jnp.float32)

    step = next(n for n in (3 * width, width) if wide % n == 0)
    parts = [slice(i, i + step) for i in range(0, wide, step)]

    load_u.wait()
    low_rank = dot(feats[...].astype(jnp.bfloat16), u_ref[...]).astype(jnp.bfloat16)
    load_v.wait()
    load_w.wait()
    pre_act = b1_ref[...]
    for part in parts:
        cross_out = dot(low_rank, v_ref[:, part]) + bias_ref[:, part]
        crossed[:, part] = cross_out
        own = feats[:, part]
        pre_act = pre_act + dot((own * cross_out + own).astype(jnp.bfloat16), w_ref[part, :])
    out_weight = out_w_ref[...].astype(jnp.float32)
    sig_act = jax.nn.sigmoid(pre_act)
    logits = jnp.sum(pre_act * sig_act * out_weight, axis=1, keepdims=True)
    row_at = lax.broadcasted_iota(jnp.int32, (rows, rows), 0)
    column_at = lax.broadcasted_iota(jnp.int32, (rows, rows), 1)
    labels = jnp.sum(
        jnp.where(row_at == column_at, label_ref[pl.ds(role, 1), :], 0.0), axis=1, keepdims=True
    )
    grad_logit = jax.nn.sigmoid(logits) - labels
    slope = sig_act * (1.0 + pre_act * (1.0 - sig_act))
    grad_act = (grad_logit * out_weight * slope).astype(jnp.bfloat16)
    grad_low = jnp.zeros((rows, u_ref.shape[1]), jnp.float32)
    for part in parts:
        grad_mixed = dot(grad_act, w_ref[part, :], NT)
        grad_cross = (grad_mixed * feats[:, part]).astype(jnp.bfloat16)
        mixed_grad[:, part] = grad_mixed * (crossed[:, part] + 1.0)
        grad_low = grad_low + dot(grad_cross, v_ref[:, part], NT)
    grad_low = grad_low.astype(jnp.bfloat16)
    for part in parts:
        total = (mixed_grad[:, part] + dot(grad_low, u_ref[part, :], NT)).astype(jnp.bfloat16)
        for i in range(step // width):
            grads[part.start // width + i] = total[:, i * width : (i + 1) * width]

    @pl.loop(0, pieces)
    def _(p):
        out_ref[p] = grads[owner_ref[p] + 1]


def dense(arrived, piece_table, dense_input, labels, cross_u, cross_v, cross_bias, top_w1, top_b1, out_w):
    pieces, rows, width = arrived.shape
    wide, rank = cross_u.shape
    hidden = top_w1.shape[1]
    vmem = pl.BlockSpec(memory_space=pltpu.VMEM)
    smem = pl.BlockSpec(memory_space=pltpu.SMEM)
    anywhere = pl.BlockSpec(memory_space=pl.ANY)
    return pl.pallas_call(
        dense_kernel,
        out_shape=jax.ShapeDtypeStruct(arrived.shape, jnp.bfloat16),
        in_specs=[smem] + [vmem] * 6 + [anywhere] * 3,
        out_specs=vmem,
        scratch_shapes=[
            pltpu.VMEM(cross_u.shape, jnp.bfloat16),
            pltpu.VMEM(cross_v.shape, jnp.bfloat16),
            pltpu.VMEM(top_w1.shape, jnp.bfloat16),
            pltpu.VMEM((rows, wide), jnp.float32),
            pltpu.VMEM((rows, wide), jnp.float32),
            pltpu.VMEM((rows, wide), jnp.float32),
            pltpu.VMEM((wide // width, rows, width), jnp.bfloat16),
            pltpu.SemaphoreType.DMA((3,)),
        ],
        compiler_params=pltpu.CompilerParams(vmem_limit_bytes=56 * 1024 * 1024),
    )(
        piece_table, arrived, dense_input, labels.reshape(2, rows), cross_bias[None], top_b1[None],
        out_w[None], cross_u, cross_v, top_w1,
    )


def local(
    table_rows, piece_table, bag_rows, bag_of, bag_weight, dense_input, labels,
    cross_u, cross_v, cross_bias, top_w1, top_b1, out_w,
):
    devices = lax.axis_size("dev")
    half = dense_input.shape[0] // 2
    pieces, _, width = table_rows.shape
    pooled = pool(table_rows, bag_rows, bag_of, bag_weight, half, devices)
    arrived = lax.all_to_all(pooled, "dev", split_axis=0, concat_axis=0, tiled=True)
    arrived = arrived.reshape(devices * pieces, half, width)
    grads = dense(
        arrived, piece_table, dense_input, labels, cross_u, cross_v, cross_bias, top_w1, top_b1, out_w
    )
    grads = grads.reshape(devices, pieces, half, width)
    returned = lax.all_to_all(grads, "dev", split_axis=0, concat_axis=0, tiled=True)
    return returned.transpose(0, 2, 1, 3)


def solution(mesh):
    split, whole = P("dev"), P()
    return jax.shard_map(
        local,
        mesh=mesh,
        in_specs=(split, whole, split, split, split, split, split) + (whole,) * 6,
        out_specs=P(None, "role", "dev", None),
        check_vma=False,
    )
```

```python
import jax
import jax.numpy as jnp
from jax import lax
from jax.experimental import pallas as pl
from jax.experimental.pallas import tpu as pltpu
from jax.sharding import PartitionSpec as P

LANES = 128
WINDOW = 384
LOW = 256
CHUNKS = 2
NT = (((1,), (1,)), ((), ()))
NN = (((1,), (0,)), ((), ()))


def dot(a, b, dims=NN):
    return lax.dot_general(a, b, dims, preferred_element_type=jnp.float32)


def pool_kernel(
    owner_ref, first_ref, last_ref, table_ref, rows_ref, bags_ref, scale_ref,
    out_ref, lead_ref, spare_ref, spare_owner_ref, flipped, scale_wide,
):
    blocks, pieces, half, width = out_ref.shape
    length = table_ref.shape[1]
    total = rows_ref.shape[1]
    groups = length // LOW
    role = lax.axis_index("role")

    @pl.loop(0, lead_ref.shape[0])
    def _(t):
        lead_ref[t] = -1

    @pl.loop(0, spare_ref.shape[0])
    def _(e):
        spare_ref[e] = 0
        spare_owner_ref[e] = -1

    def assign(p, used):
        t = owner_ref[p]
        again = lead_ref[t] >= 0

        @pl.when(again)
        def _():
            spare_ref[used] = p
            spare_owner_ref[used] = t

        @pl.when(jnp.logical_not(again))
        def _():
            lead_ref[t] = p

        return used + again.astype(jnp.int32)

    lax.fori_loop(0, owner_ref.shape[0], assign, jnp.int32(0))
    scale_wide[...] = scale_ref[...].astype(jnp.float32)
    for p in range(pieces):
        for g in range(groups):
            flipped[p, g * width : (g + 1) * width, :] = (
                table_ref[p, g * LOW : (g + 1) * LOW, :].astype(jnp.float32).T.astype(jnp.bfloat16)
            )
    low_ids = lax.broadcasted_iota(jnp.int32, (LOW, WINDOW), 0)
    bag_ids = lax.broadcasted_iota(jnp.int32, (half, WINDOW), 0)
    places = lax.broadcasted_iota(jnp.int32, (1, WINDOW), 1)

    def window(p, base, begin, first_bag):
        start = pl.multiple_of(jnp.minimum(begin, total - WINDOW), LANES)
        span = pl.ds(start, WINDOW)
        ids = rows_ref[pl.ds(p, 1), span]
        bags = bags_ref[pl.ds(p, 1), span] - first_bag
        bags = jnp.where(places + start >= begin, bags, -1)
        scale = scale_wide[pl.ds(p, 1), span]
        low, high = ids % LOW, ids // LOW
        hot = jnp.where(low_ids == low, 1.0, 0.0).astype(jnp.bfloat16)
        picked = dot(flipped[p, :width, :], hot)
        for g in range(1, groups):
            picked = jnp.where(high == g, dot(flipped[p, g * width : (g + 1) * width, :], hot), picked)
        spread = jnp.where(bag_ids == bags, scale, 0.0).astype(jnp.bfloat16)
        return dot(spread, picked.astype(jnp.bfloat16), NT)

    @pl.loop(0, blocks)
    def _(k):
        first_bag = (2 * k + role) * half
        bases = [first_ref[p, k] // LANES * LANES for p in range(pieces)]
        sums = [window(p, bases[p], bases[p], first_bag) for p in range(pieces)]
        for p in range(pieces):
            out_ref[k, p] = sums[p].astype(jnp.bfloat16)
        for p in range(pieces):
            count = (last_ref[p, k] - bases[p] + WINDOW - 1) // WINDOW

            @pl.when(count > 1)
            def _():
                def more(j, acc):
                    return acc + window(p, bases[p], bases[p] + j * WINDOW, first_bag)

                first = window(p, bases[p], bases[p], first_bag)
                out_ref[k, p] = lax.fori_loop(1, count, more, first).astype(jnp.bfloat16)


def pool(piece_table, table_rows, bag_rows, bag_of, bag_weight, half, blocks, tables):
    pieces, length, width = table_rows.shape
    role = lax.axis_index("role")
    edges = (2 * jnp.arange(blocks, dtype=jnp.int32) + role) * half
    first = jnp.sum((bag_of[:, None, :] < edges[None, :, None]).astype(jnp.int32), axis=2)
    last = jnp.sum((bag_of[:, None, :] < edges[None, :, None] + half).astype(jnp.int32), axis=2)
    spares = max(1, piece_table.shape[0] - tables)
    vmem = pl.BlockSpec(memory_space=pltpu.VMEM)
    smem = pl.BlockSpec(memory_space=pltpu.SMEM)
    return pl.pallas_call(
        pool_kernel,
        out_shape=[
            jax.ShapeDtypeStruct((blocks, pieces, half, width), jnp.bfloat16),
            jax.ShapeDtypeStruct((tables,), jnp.int32),
            jax.ShapeDtypeStruct((spares,), jnp.int32),
            jax.ShapeDtypeStruct((spares,), jnp.int32),
        ],
        in_specs=[smem, smem, smem, vmem, vmem, vmem, vmem],
        out_specs=[vmem, smem, smem, smem],
        scratch_shapes=[
            pltpu.VMEM((pieces, length // LOW * width, LOW), jnp.bfloat16),
            pltpu.VMEM(bag_weight.shape, jnp.float32),
        ],
        compiler_params=pltpu.CompilerParams(vmem_limit_bytes=40 * 1024 * 1024),
    )(piece_table, first, last, table_rows, bag_rows, bag_of, bag_weight)


def dense_kernel(
    owner_ref, lead_ref, spare_ref, spare_owner_ref, pooled_ref, dense_ref, label_ref, bias_ref, b1_ref,
    out_w_ref, u_hbm, v_hbm, w_hbm, out_ref,
    u_ref, v_ref, w_ref, feats, crossed, mixed_grad, grads, arrived, outgoing,
    sems, there_send, there_recv, back_send, back_recv,
):
    devices, local_pieces, half, width = pooled_ref.shape
    pieces = devices * local_pieces
    rows, wide = feats.shape
    tables = wide // width - 1
    role = lax.axis_index("role")
    me = lax.axis_index("dev")
    load_u = pltpu.make_async_copy(u_hbm, u_ref, sems.at[0])
    load_v = pltpu.make_async_copy(v_hbm, v_ref, sems.at[1])
    load_w = pltpu.make_async_copy(w_hbm, w_ref, sems.at[2])

    barrier = pltpu.get_barrier_semaphore()

    @pl.loop(1, devices)
    def _(s):
        pl.semaphore_signal(
            barrier, inc=1, device_id={"dev": (me + s) % devices}, device_id_type=pl.DeviceIdType.MESH
        )

    load_u.start()
    load_v.start()
    load_w.start()
    pl.semaphore_wait(barrier, devices - 1)

    def there(c, s):
        peer = (me + s) % devices
        return pltpu.make_async_remote_copy(
            src_ref=pooled_ref.at[peer, :, c * rows : (c + 1) * rows, :],
            dst_ref=arrived[c].at[me],
            send_sem=there_send.at[c, s],
            recv_sem=there_recv.at[c, s],
            device_id={"dev": peer},
            device_id_type=pl.DeviceIdType.MESH,
        )

    def back(c, s):
        peer = (me + s) % devices
        return pltpu.make_async_remote_copy(
            src_ref=outgoing[c].at[peer],
            dst_ref=out_ref.at[me, :, c * rows : (c + 1) * rows, :],
            send_sem=back_send.at[c, s],
            recv_sem=back_recv.at[c, s],
            device_id={"dev": peer},
            device_id_type=pl.DeviceIdType.MESH,
        )

    for c in range(CHUNKS):

        @pl.loop(1, devices)
        def _(s):
            there(c, s).start()

    for c in range(CHUNKS):
        arrived[c][me] = pooled_ref[me, :, c * rows : (c + 1) * rows, :]

    step = next(n for n in (3 * width, width) if wide % n == 0)
    parts = [slice(i, i + step) for i in range(0, wide, step)]
    out_weight = out_w_ref[...].astype(jnp.float32)
    row_at = lax.broadcasted_iota(jnp.int32, (rows, rows), 0)
    column_at = lax.broadcasted_iota(jnp.int32, (rows, rows), 1)
    spares = pieces - tables

    for c in range(CHUNKS):
        feats[:, :width] = dense_ref[pl.ds(pl.multiple_of(role * half + c * rows, rows), rows), :].astype(jnp.float32)

        @pl.loop(1, devices)
        def _(s):
            there(c, s).wait_recv()

        def piece(index):
            return arrived[c][index // local_pieces, index % local_pieces].astype(jnp.float32)

        @pl.loop(0, tables)
        def _(t):
            def add(e, acc):
                return acc + piece(spare_ref[e]) * jnp.where(spare_owner_ref[e] == t, 1.0, 0.0)

            acc = piece(lead_ref[t])
            if spares <= 16:
                for e in range(spares):
                    acc = add(e, acc)
            else:
                acc = lax.fori_loop(0, spares, add, acc)
            feats[:, pl.ds(pl.multiple_of((t + 1) * width, width), width)] = acc

        if c == 0:
            load_u.wait()
        low_rank = dot(feats[...].astype(jnp.bfloat16), u_ref[...]).astype(jnp.bfloat16)
        if c == 0:
            load_v.wait()
            load_w.wait()
        pre_act = b1_ref[...]
        for part in parts:
            cross_out = dot(low_rank, v_ref[:, part]) + bias_ref[:, part]
            crossed[:, part] = cross_out
            own = feats[:, part]
            pre_act = pre_act + dot((own * cross_out + own).astype(jnp.bfloat16), w_ref[part, :])
        sig_act = jax.nn.sigmoid(pre_act)
        logits = jnp.sum(pre_act * sig_act * out_weight, axis=1, keepdims=True)
        labels = jnp.sum(
            jnp.where(row_at == column_at, label_ref[pl.ds(role * CHUNKS + c, 1), :], 0.0),
            axis=1,
            keepdims=True,
        )
        grad_logit = jax.nn.sigmoid(logits) - labels
        slope = sig_act * (1.0 + pre_act * (1.0 - sig_act))
        grad_act = (grad_logit * out_weight * slope).astype(jnp.bfloat16)
        grad_low = jnp.zeros((rows, u_ref.shape[1]), jnp.float32)
        for part in parts:
            grad_mixed = dot(grad_act, w_ref[part, :], NT)
            grad_cross = (grad_mixed * feats[:, part]).astype(jnp.bfloat16)
            mixed_grad[:, part] = grad_mixed * (crossed[:, part] + 1.0)
            grad_low = grad_low + dot(grad_cross, v_ref[:, part], NT)
        grad_low = grad_low.astype(jnp.bfloat16)
        for part in parts:
            total = (mixed_grad[:, part] + dot(grad_low, u_ref[part, :], NT)).astype(jnp.bfloat16)
            for i in range(step // width):
                grads[part.start // width + i] = total[:, i * width : (i + 1) * width]

        @pl.loop(0, devices)
        def _(d):
            for i in range(local_pieces):
                outgoing[c][d, i] = grads[owner_ref[d * local_pieces + i] + 1]

        @pl.loop(1, devices)
        def _(s):
            back(c, s).start()

        out_ref[me, :, c * rows : (c + 1) * rows, :] = outgoing[c][me]

    for c in range(CHUNKS):

        @pl.loop(1, devices)
        def _(s):
            there(c, s).wait_send()
            back(c, s).wait_send()
            back(c, s).wait_recv()


def dense(chosen, pooled, piece_table, dense_input, labels, cross_u, cross_v, cross_bias, top_w1, top_b1, out_w):
    devices, local_pieces, half, width = pooled.shape
    rows = half // CHUNKS
    wide = cross_u.shape[0]
    vmem = pl.BlockSpec(memory_space=pltpu.VMEM)
    smem = pl.BlockSpec(memory_space=pltpu.SMEM)
    anywhere = pl.BlockSpec(memory_space=pl.ANY)
    block = pltpu.VMEM((devices, local_pieces, rows, width), jnp.bfloat16)
    return pl.pallas_call(
        dense_kernel,
        out_shape=jax.ShapeDtypeStruct(pooled.shape, jnp.bfloat16),
        in_specs=[smem] * 4 + [vmem] * 6 + [anywhere] * 3,
        out_specs=vmem,
        scratch_shapes=[
            pltpu.VMEM(cross_u.shape, jnp.bfloat16),
            pltpu.VMEM(cross_v.shape, jnp.bfloat16),
            pltpu.VMEM(top_w1.shape, jnp.bfloat16),
            pltpu.VMEM((rows, wide), jnp.float32),
            pltpu.VMEM((rows, wide), jnp.float32),
            pltpu.VMEM((rows, wide), jnp.float32),
            pltpu.VMEM((wide // width, rows, width), jnp.bfloat16),
            [block] * CHUNKS,
            [block] * CHUNKS,
            pltpu.SemaphoreType.DMA((3,)),
        ]
        + [pltpu.SemaphoreType.DMA((CHUNKS, devices))] * 4,
        compiler_params=pltpu.CompilerParams(
            vmem_limit_bytes=56 * 1024 * 1024, collective_id=0, has_side_effects=True
        ),
    )(
        piece_table, *chosen, pooled, dense_input, labels.reshape(2 * CHUNKS, rows), cross_bias[None],
        top_b1[None], out_w[None], cross_u, cross_v, top_w1,
    )


def local(
    table_rows, piece_table, bag_rows, bag_of, bag_weight, dense_input, labels,
    cross_u, cross_v, cross_bias, top_w1, top_b1, out_w,
):
    devices = lax.axis_size("dev")
    half = dense_input.shape[0] // 2
    tables = cross_bias.shape[0] // dense_input.shape[1] - 1
    pooled, *chosen = pool(piece_table, table_rows, bag_rows, bag_of, bag_weight, half, devices, tables)
    returned = dense(
        chosen, pooled, piece_table, dense_input, labels, cross_u, cross_v, cross_bias, top_w1, top_b1, out_w
    )
    return returned.transpose(0, 2, 1, 3)


def solution(mesh):
    split, whole = P("dev"), P()
    return jax.shard_map(
        local,
        mesh=mesh,
        in_specs=(split, whole, split, split, split, split, split) + (whole,) * 6,
        out_specs=P(None, "role", "dev", None),
        check_vma=False,
    )
```

```python
import jax
import jax.numpy as jnp
from jax import lax
from jax.experimental import pallas as pl
from jax.experimental.pallas import tpu as pltpu
from jax.sharding import PartitionSpec as P

LANES = 128
WINDOW = 384
LOW = 256
CHUNKS = 2
NT = (((1,), (1,)), ((), ()))
NN = (((1,), (0,)), ((), ()))


def dot(a, b, dims=NN):
    return lax.dot_general(a, b, dims, preferred_element_type=jnp.float32)


def pool_kernel(
    owner_ref, first_ref, last_ref, table_ref, rows_ref, bags_ref, scale_ref,
    out_ref, lead_ref, spare_ref, spare_owner_ref, flipped, scale_wide,
):
    blocks, pieces, half, width = out_ref.shape
    length = table_ref.shape[1]
    total = rows_ref.shape[1]
    groups = length // LOW
    role = lax.axis_index("role")

    @pl.loop(0, lead_ref.shape[0])
    def _(t):
        lead_ref[t] = -1

    @pl.loop(0, spare_ref.shape[0])
    def _(e):
        spare_ref[e] = 0
        spare_owner_ref[e] = -1

    def assign(p, used):
        t = owner_ref[p]
        again = lead_ref[t] >= 0

        @pl.when(again)
        def _():
            spare_ref[used] = p
            spare_owner_ref[used] = t

        @pl.when(jnp.logical_not(again))
        def _():
            lead_ref[t] = p

        return used + again.astype(jnp.int32)

    lax.fori_loop(0, owner_ref.shape[0], assign, jnp.int32(0))
    scale_wide[...] = scale_ref[...].astype(jnp.float32)
    for p in range(pieces):
        for g in range(groups):
            flipped[p, g * width : (g + 1) * width, :] = (
                table_ref[p, g * LOW : (g + 1) * LOW, :].astype(jnp.float32).T.astype(jnp.bfloat16)
            )
    low_ids = lax.broadcasted_iota(jnp.int32, (LOW, WINDOW), 0)
    bag_ids = lax.broadcasted_iota(jnp.int32, (half, WINDOW), 0)
    places = lax.broadcasted_iota(jnp.int32, (1, WINDOW), 1)

    def window(p, base, begin, first_bag):
        start = pl.multiple_of(jnp.minimum(begin, total - WINDOW), LANES)
        span = pl.ds(start, WINDOW)
        ids = rows_ref[pl.ds(p, 1), span]
        bags = bags_ref[pl.ds(p, 1), span] - first_bag
        bags = jnp.where(places + start >= begin, bags, -1)
        scale = scale_wide[pl.ds(p, 1), span]
        low, high = ids % LOW, ids // LOW
        hot = jnp.where(low_ids == low, 1.0, 0.0).astype(jnp.bfloat16)
        picked = dot(flipped[p, :width, :], hot)
        for g in range(1, groups):
            picked = jnp.where(high == g, dot(flipped[p, g * width : (g + 1) * width, :], hot), picked)
        spread = jnp.where(bag_ids == bags, scale, 0.0).astype(jnp.bfloat16)
        return dot(spread, picked.astype(jnp.bfloat16), NT)

    @pl.loop(0, blocks)
    def _(k):
        first_bag = (2 * k + role) * half
        bases = [first_ref[p, k] // LANES * LANES for p in range(pieces)]
        sums = [window(p, bases[p], bases[p], first_bag) for p in range(pieces)]
        for p in range(pieces):
            out_ref[k, p] = sums[p].astype(jnp.bfloat16)
        for p in range(pieces):
            count = (last_ref[p, k] - bases[p] + WINDOW - 1) // WINDOW

            @pl.when(count > 1)
            def _():
                def more(j, acc):
                    return acc + window(p, bases[p], bases[p] + j * WINDOW, first_bag)

                first = window(p, bases[p], bases[p], first_bag)
                out_ref[k, p] = lax.fori_loop(1, count, more, first).astype(jnp.bfloat16)


def pool(piece_table, table_rows, bag_rows, bag_of, bag_weight, half, blocks, tables):
    pieces, length, width = table_rows.shape
    role = lax.axis_index("role")
    edges = (2 * jnp.arange(blocks, dtype=jnp.int32) + role) * half
    first = jnp.sum((bag_of[:, None, :] < edges[None, :, None]).astype(jnp.int32), axis=2)
    last = jnp.sum((bag_of[:, None, :] < edges[None, :, None] + half).astype(jnp.int32), axis=2)
    spares = max(1, piece_table.shape[0] - tables)
    vmem = pl.BlockSpec(memory_space=pltpu.VMEM)
    smem = pl.BlockSpec(memory_space=pltpu.SMEM)
    return pl.pallas_call(
        pool_kernel,
        out_shape=[
            jax.ShapeDtypeStruct((blocks, pieces, half, width), jnp.bfloat16),
            jax.ShapeDtypeStruct((tables,), jnp.int32),
            jax.ShapeDtypeStruct((spares,), jnp.int32),
            jax.ShapeDtypeStruct((spares,), jnp.int32),
        ],
        in_specs=[smem, smem, smem, vmem, vmem, vmem, vmem],
        out_specs=[vmem, smem, smem, smem],
        scratch_shapes=[
            pltpu.VMEM((pieces, length // LOW * width, LOW), jnp.bfloat16),
            pltpu.VMEM(bag_weight.shape, jnp.float32),
        ],
        compiler_params=pltpu.CompilerParams(vmem_limit_bytes=40 * 1024 * 1024),
    )(piece_table, first, last, table_rows, bag_rows, bag_of, bag_weight)


def dense_kernel(
    owner_ref, lead_ref, spare_ref, spare_owner_ref, pooled_ref, dense_ref, label_ref, bias_ref, b1_ref,
    out_w_ref, u_hbm, v_hbm, w_hbm, out_ref,
    u_ref, v_ref, w_ref, feats, crossed, mixed_grad, grads, arrived, outgoing,
    sems, there_send, there_recv, back_send, back_recv,
):
    devices, local_pieces, half, width = pooled_ref.shape
    pieces = devices * local_pieces
    rows, wide = feats.shape
    tables = wide // width - 1
    role = lax.axis_index("role")
    me = lax.axis_index("dev")
    load_u = pltpu.make_async_copy(u_hbm, u_ref, sems.at[0])
    load_v = pltpu.make_async_copy(v_hbm, v_ref, sems.at[1])
    load_w = pltpu.make_async_copy(w_hbm, w_ref, sems.at[2])

    barrier = pltpu.get_barrier_semaphore()

    @pl.loop(1, devices)
    def _(s):
        pl.semaphore_signal(
            barrier, inc=1, device_id={"dev": (me + s) % devices}, device_id_type=pl.DeviceIdType.MESH
        )

    load_u.start()
    load_v.start()
    load_w.start()
    pl.semaphore_wait(barrier, devices - 1)

    def there(c, s):
        peer = (me + s) % devices
        return pltpu.make_async_remote_copy(
            src_ref=pooled_ref.at[peer, :, c * rows : (c + 1) * rows, :],
            dst_ref=arrived[c].at[me],
            send_sem=there_send.at[c, s],
            recv_sem=there_recv.at[c, s],
            device_id={"dev": peer},
            device_id_type=pl.DeviceIdType.MESH,
        )

    def back(c, s):
        peer = (me + s) % devices
        return pltpu.make_async_remote_copy(
            src_ref=outgoing[c].at[peer],
            dst_ref=out_ref.at[me, :, c * rows : (c + 1) * rows, :],
            send_sem=back_send.at[c, s],
            recv_sem=back_recv.at[c, s],
            device_id={"dev": peer},
            device_id_type=pl.DeviceIdType.MESH,
        )

    for c in range(CHUNKS):

        @pl.loop(1, devices)
        def _(s):
            there(c, s).start()

    for c in range(CHUNKS):
        arrived[c][me] = pooled_ref[me, :, c * rows : (c + 1) * rows, :]

    step = next(n for n in (3 * width, width) if wide % n == 0)
    parts = [slice(i, i + step) for i in range(0, wide, step)]
    out_weight = out_w_ref[...].astype(jnp.float32)[None, :]
    row_at = lax.broadcasted_iota(jnp.int32, (rows, 2 * half), 0)
    column_at = lax.broadcasted_iota(jnp.int32, (rows, 2 * half), 1)
    spares = pieces - tables

    for c in range(CHUNKS):
        feats[:, :width] = dense_ref[pl.ds(pl.multiple_of(role * half + c * rows, rows), rows), :].astype(jnp.float32)

        @pl.loop(1, devices)
        def _(s):
            there(c, s).wait_recv()

        def piece(index):
            return arrived[c][index // local_pieces, index % local_pieces].astype(jnp.float32)

        @pl.loop(0, tables)
        def _(t):
            def add(e, acc):
                return acc + piece(spare_ref[e]) * jnp.where(spare_owner_ref[e] == t, 1.0, 0.0)

            acc = piece(lead_ref[t])
            if spares <= 16:
                for e in range(spares):
                    acc = add(e, acc)
            else:
                acc = lax.fori_loop(0, spares, add, acc)
            feats[:, pl.ds(pl.multiple_of((t + 1) * width, width), width)] = acc

        if c == 0:
            load_u.wait()
        low_rank = dot(feats[...].astype(jnp.bfloat16), u_ref[...]).astype(jnp.bfloat16)
        if c == 0:
            load_v.wait()
            load_w.wait()
        pre_act = b1_ref[...][None, :]
        for part in parts:
            cross_out = dot(low_rank, v_ref[:, part]) + bias_ref[part][None, :]
            crossed[:, part] = cross_out
            own = feats[:, part]
            pre_act = pre_act + dot((own * cross_out + own).astype(jnp.bfloat16), w_ref[part, :])
        sig_act = jax.nn.sigmoid(pre_act)
        logits = jnp.sum(pre_act * sig_act * out_weight, axis=1, keepdims=True)
        labels = jnp.sum(
            jnp.where(row_at + (role * half + c * rows) == column_at, label_ref[...][None, :], 0.0),
            axis=1,
            keepdims=True,
        )
        grad_logit = jax.nn.sigmoid(logits) - labels
        slope = sig_act * (1.0 + pre_act * (1.0 - sig_act))
        grad_act = (grad_logit * out_weight * slope).astype(jnp.bfloat16)
        grad_low = jnp.zeros((rows, u_ref.shape[1]), jnp.float32)
        for part in parts:
            grad_mixed = dot(grad_act, w_ref[part, :], NT)
            grad_cross = (grad_mixed * feats[:, part]).astype(jnp.bfloat16)
            mixed_grad[:, part] = grad_mixed * (crossed[:, part] + 1.0)
            grad_low = grad_low + dot(grad_cross, v_ref[:, part], NT)
        grad_low = grad_low.astype(jnp.bfloat16)
        for part in parts:
            total = (mixed_grad[:, part] + dot(grad_low, u_ref[part, :], NT)).astype(jnp.bfloat16)
            for i in range(step // width):
                grads[part.start // width + i] = total[:, i * width : (i + 1) * width]

        @pl.loop(0, devices)
        def _(d):
            for i in range(local_pieces):
                outgoing[c][d, i] = grads[owner_ref[d * local_pieces + i] + 1]

        @pl.loop(1, devices)
        def _(s):
            back(c, s).start()

        out_ref[me, :, c * rows : (c + 1) * rows, :] = outgoing[c][me]

    for c in range(CHUNKS):

        @pl.loop(1, devices)
        def _(s):
            there(c, s).wait_send()
            back(c, s).wait_send()
            back(c, s).wait_recv()


def dense(chosen, pooled, piece_table, dense_input, labels, cross_u, cross_v, cross_bias, top_w1, top_b1, out_w):
    devices, local_pieces, half, width = pooled.shape
    rows = half // CHUNKS
    wide = cross_u.shape[0]
    vmem = pl.BlockSpec(memory_space=pltpu.VMEM)
    smem = pl.BlockSpec(memory_space=pltpu.SMEM)
    anywhere = pl.BlockSpec(memory_space=pl.ANY)
    block = pltpu.VMEM((devices, local_pieces, rows, width), jnp.bfloat16)
    return pl.pallas_call(
        dense_kernel,
        out_shape=jax.ShapeDtypeStruct(pooled.shape, jnp.bfloat16),
        in_specs=[smem] * 4 + [vmem] * 6 + [anywhere] * 3,
        out_specs=vmem,
        scratch_shapes=[
            pltpu.VMEM(cross_u.shape, jnp.bfloat16),
            pltpu.VMEM(cross_v.shape, jnp.bfloat16),
            pltpu.VMEM(top_w1.shape, jnp.bfloat16),
            pltpu.VMEM((rows, wide), jnp.float32),
            pltpu.VMEM((rows, wide), jnp.float32),
            pltpu.VMEM((rows, wide), jnp.float32),
            pltpu.VMEM((wide // width, rows, width), jnp.bfloat16),
            [block] * CHUNKS,
            [block] * CHUNKS,
            pltpu.SemaphoreType.DMA((3,)),
        ]
        + [pltpu.SemaphoreType.DMA((CHUNKS, devices))] * 4,
        compiler_params=pltpu.CompilerParams(
            vmem_limit_bytes=56 * 1024 * 1024, collective_id=0, has_side_effects=True
        ),
    )(
        piece_table, *chosen, pooled, dense_input, labels, cross_bias,
        top_b1, out_w, cross_u, cross_v, top_w1,
    )


def local(
    table_rows, piece_table, bag_rows, bag_of, bag_weight, dense_input, labels,
    cross_u, cross_v, cross_bias, top_w1, top_b1, out_w,
):
    devices = lax.axis_size("dev")
    half = dense_input.shape[0] // 2
    tables = cross_bias.shape[0] // dense_input.shape[1] - 1
    pooled, *chosen = pool(piece_table, table_rows, bag_rows, bag_of, bag_weight, half, devices, tables)
    returned = dense(
        chosen, pooled, piece_table, dense_input, labels, cross_u, cross_v, cross_bias, top_w1, top_b1, out_w
    )
    return returned.transpose(0, 2, 1, 3)


def solution(mesh):
    split, whole = P("dev"), P()
    return jax.shard_map(
        local,
        mesh=mesh,
        in_specs=(split, whole, split, split, split, split, split) + (whole,) * 6,
        out_specs=P(None, "role", "dev", None),
        check_vma=False,
    )
```
